8 devices in a mesh: data: 2 (over z, y), seq: 4 (over x, core).
Axes of the slice: x: 2, y: 2, z: 1, core: 2. Of those that a mesh axis runs over, the one named last changes fastest.
Arguments:
- tokens: bfloat16 [64, 4096, 768], P('data', 'seq'), parts along dimension 0
- lengths: int32 [64], P('data'), parts along dimension 0
- slot_params: bfloat16 [768, 128], replicated
- logit_scale: float32 [1], replicated
- w_in: bfloat16 [64, 768, 3072], P('seq')
- w_out: bfloat16 [64, 3072, 768], P('seq')
Outputs:
- output: bfloat16 [64, 4096, 768], P('data', 'seq'), parts along dimension 0
There are 2 independent parts. The reference program is written for one: setup_inputs(seed, part) draws one part's arguments, and reference() takes and returns one part's arrays. A program takes and returns all parts, laid end to end along the dimension named above; an argument that names none is the same for every part.
All inputs are finite; a program needn't handle non-finite values.
Results may differ from the reference program's by a relative error of at most 0.0148089.
Values are sent between devices in bfloat16 or wider.
A program may use at most 1 GiB of HBM per device.

```python
import jax
import jax.numpy as jnp
from jax import lax

BATCH = 32
TOKENS = 4096
D_MODEL = 768
FF_DIM = 3072
EXPERTS = 64
SLOTS = 2
NUM_SLOTS = EXPERTS * SLOTS


def setup_inputs(seed: int = 0, part: int = 0) -> dict:
    base_key = jax.random.key(seed)
    k_phi, k_win, k_wout, k_gain = jax.random.split(base_key, 4)
    part_key = jax.random.fold_in(base_key, part)
    k_sel, k_noise, k_len = jax.random.split(part_key, 3)
    slot_params = jax.random.normal(k_phi, (D_MODEL, NUM_SLOTS), jnp.float32)
    chosen = jax.random.randint(k_sel, (BATCH, TOKENS), 0, NUM_SLOTS)
    noise = jax.random.normal(k_noise, (BATCH, TOKENS, D_MODEL), jnp.float32)
    tokens = jnp.take(slot_params.T, chosen, axis=0) + noise
    lengths = jax.random.randint(k_len, (BATCH,), 1, TOKENS + 1)
    logit_scale = jax.random.uniform(k_gain, (1,), jnp.float32, 6.0, 9.0)
    w_in = jax.random.normal(k_win, (EXPERTS, D_MODEL, FF_DIM), jnp.float32) * D_MODEL ** -0.5
    w_out = jax.random.normal(k_wout, (EXPERTS, FF_DIM, D_MODEL), jnp.float32) * FF_DIM ** -0.5
    return {
        "tokens": tokens.astype(jnp.bfloat16),
        "lengths": lengths.astype(jnp.int32),
        "slot_params": slot_params.astype(jnp.bfloat16),
        "logit_scale": logit_scale,
        "w_in": w_in.astype(jnp.bfloat16),
        "w_out": w_out.astype(jnp.bfloat16),
    }


def reference(tokens, lengths, slot_params, logit_scale, w_in, w_out):
    params_f32 = slot_params.astype(jnp.float32)
    col_inv = lax.rsqrt(jnp.sum(params_f32 * params_f32, axis=0, keepdims=True) + 1e-6)
    phi_norm = (params_f32 * (logit_scale[0] * col_inv)).astype(jnp.bfloat16)
    positions = jnp.arange(TOKENS)

    def row_logits(row_tokens):
        tok_f32 = row_tokens.astype(jnp.float32)
        tok_norm = (tok_f32 * lax.rsqrt(jnp.sum(tok_f32 * tok_f32, axis=-1, keepdims=True) + 1e-6)).astype(jnp.bfloat16)
        return jnp.dot(tok_norm, phi_norm, preferred_element_type=jnp.float32)

    def dispatch_row(row_args):
        row_tokens, row_len = row_args
        logits = row_logits(row_tokens)
        is_valid = (positions < row_len)[:, None]
        col_max = jnp.max(jnp.where(is_valid, logits, -jnp.inf), axis=0)
        disp_w = jnp.where(is_valid, jnp.exp(logits - col_max[None, :]), 0.0)
        col_sum = jnp.sum(disp_w, axis=0)
        slot_sum = jnp.dot(disp_w.astype(jnp.bfloat16).T, row_tokens, preferred_element_type=jnp.float32)
        return (slot_sum / col_sum[:, None]).astype(jnp.bfloat16)

    slot_in = lax.map(dispatch_row, (tokens, lengths))
    by_expert = slot_in.reshape(BATCH, EXPERTS, SLOTS, D_MODEL).transpose(1, 0, 2, 3).reshape(EXPERTS, BATCH * SLOTS, D_MODEL)

    def expert_ffn(exp_args):
        exp_in, exp_w_in, exp_w_out = exp_args
        hidden = jax.nn.gelu(jnp.dot(exp_in, exp_w_in, preferred_element_type=jnp.float32)).astype(jnp.bfloat16)
        return jnp.dot(hidden, exp_w_out, preferred_element_type=jnp.float32).astype(jnp.bfloat16)

    expert_out = lax.map(expert_ffn, (by_expert, w_in, w_out))
    slot_out = expert_out.reshape(EXPERTS, BATCH, SLOTS, D_MODEL).transpose(1, 0, 2, 3).reshape(BATCH, NUM_SLOTS, D_MODEL)

    def combine_row(row_args):
        row_tokens, row_len, row_slots = row_args
        logits = row_logits(row_tokens)
        is_valid = (positions < row_len)[:, None]
        combine_w = jax.nn.softmax(logits, axis=-1).astype(jnp.bfloat16)
        mixed = jnp.dot(combine_w, row_slots, preferred_element_type=jnp.float32).astype(jnp.bfloat16)
        return jnp.where(is_valid, mixed, jnp.zeros_like(mixed))

    return lax.map(combine_row, (tokens, lengths, slot_out))
```

```python
import functools

import jax
import jax.numpy as jnp
from jax import lax
from jax.experimental import pallas as pl
from jax.experimental.pallas import tpu as pltpu
from jax.sharding import PartitionSpec as P

BLK = 256
TS = 4
WS = 4
FC = 512
G = 16


def _swap_matrix():
    r = lax.broadcasted_iota(jnp.int32, (G * G, G * G), 0)
    c = lax.broadcasted_iota(jnp.int32, (G * G, G * G), 1)
    hit = ((r >> 4) == (c & 15)) & ((r & 15) == (c >> 4))
    return jnp.where(hit, 1.0, 0.0).astype(jnp.bfloat16)


def _front_kernel(rows, experts, len_ref, scale_ref, phi_ref, x_hbm, win_hbm, wout_hbm,
                  ys_hbm, ct_hbm,
                  xbuf, phit, wt, ctst, sbuf, rbuf, qbuf, xst, zt, zr, zs, yst, w1, w2,
                  tok_sem, ct_sem, w_sem, z_ssem, z_rsem,
                  d_ssem, d_rsem, x_ssem, x_rsem,
                  l_sem, c_ssem, c_rsem, p_ssem, p_rsem, f_ssem, f_rsem):
    toks, width = x_hbm.shape[1], x_hbm.shape[2]
    slots = phi_ref.shape[1]
    own = sbuf.shape[3]
    per = own // experts
    me = lax.axis_index("seq")
    xi = me // 2
    ci = me % 2
    core_peer = 2 * xi + (1 - ci)
    x_peer = 2 * (1 - xi) + ci
    diag = 2 * (1 - xi) + (1 - ci)

    def remote(src, dst, ssem, rsem, dev):
        return pltpu.make_async_remote_copy(
            src_ref=src, dst_ref=dst, send_sem=ssem, recv_sem=rsem,
            device_id={"seq": dev}, device_id_type=pl.DeviceIdType.MESH)

    def tok_copy(b):
        return pltpu.make_async_copy(x_hbm.at[b], xbuf.at[b % TS], tok_sem.at[b % TS])

    def ct_copy(b):
        return pltpu.make_async_copy(ctst.at[b % 2], ct_hbm.at[b], ct_sem.at[b % 2])

    def w1_copy(e):
        return pltpu.make_async_copy(win_hbm.at[e], w1.at[e % WS], w_sem.at[e % WS, 0])

    def w2_copy(e):
        return pltpu.make_async_copy(wout_hbm.at[e], w2.at[e % WS], w_sem.at[e % WS, 1])

    def d_copy(b):
        return remote(sbuf.at[b, :, 1 - ci], rbuf.at[b], d_ssem.at[b], d_rsem.at[b], core_peer)

    def x_copy(b):
        return remote(rbuf.at[b, 1 - xi], qbuf.at[b], x_ssem.at[b], x_rsem.at[b], x_peer)

    def z_copies():
        out = []
        for k, dev in enumerate((core_peer, x_peer, diag)):
            out.append(remote(zt.at[pl.ds(pl.multiple_of(dev * own, own), own)], zr.at[k],
                              z_ssem.at[k], z_rsem.at[k], dev))
        return out

    barrier = pltpu.get_barrier_semaphore()
    for dev in (core_peer, x_peer, diag):
        pl.semaphore_signal(barrier, inc=1, device_id={"seq": dev}, device_id_type=pl.DeviceIdType.MESH)
    for k in range(TS - 1):
        tok_copy(k).start()

    scale = scale_ref[0]
    phi = phi_ref[...].astype(jnp.float32)
    col_inv = lax.rsqrt(jnp.sum(phi * phi, axis=0, keepdims=True) + 1e-6)
    phit[...] = (phi * (scale * col_inv)).T.astype(jnp.bfloat16)
    zt[...] = jnp.zeros_like(zt)

    def gate(b):
        limit = len_ref[b] - me * toks
        zacc = None
        for k in range(toks // BLK):
            cols = pl.ds(k * BLK, BLK)
            xf = xbuf[b % TS, cols, :].astype(jnp.float32)
            inv = lax.rsqrt(jnp.sum(xf * xf, axis=1, keepdims=True) + 1e-6)
            xn = (xf * inv).astype(jnp.bfloat16)
            lt = lax.dot_general(phit[...], xn, (((1,), (1,)), ((), ())),
                                 preferred_element_type=jnp.float32)
            e = jnp.exp(lt - scale)
            den = jnp.sum(e, axis=0, keepdims=True)
            ctst[b % 2, :, cols] = (e * (1.0 / den)).astype(jnp.bfloat16)
            pos = lax.broadcasted_iota(jnp.int32, (1, BLK), 1) + k * BLK
            w = jnp.where(pos < limit, e, 0.0)
            wt[:, cols] = w.astype(jnp.bfloat16)
            for h in range(BLK // 128):
                part = w[:, h * 128:(h + 1) * 128]
                zacc = part if zacc is None else zacc + part
        zcol = jnp.sum(zacc, axis=1, keepdims=True)
        lane = lax.broadcasted_iota(jnp.int32, zt.shape, 1)
        zt[...] = jnp.where(lane == b, zcol, zt[...])

    def sums(b):
        s = jnp.dot(wt[...], xbuf[b % TS], preferred_element_type=jnp.float32)
        sbuf[b] = s.astype(jnp.bfloat16).reshape(2, 2, own, width)

    def mid(b):
        for h in range(2):
            rbuf[b, h] = (rbuf[b, h].astype(jnp.float32)
                          + sbuf[b, h, ci].astype(jnp.float32)).astype(jnp.bfloat16)

    tok_copy(0).wait()
    gate(0)
    ct_copy(0).start()
    pl.semaphore_wait(barrier, 3)

    def step(b, _):
        @pl.when(b >= 2)
        def _():
            d_copy(b - 2).start()

        @pl.when(b >= 5)
        def _():
            x_copy(b - 5).start()

        @pl.when(b >= 4)
        def _():
            d_copy(b - 4).wait_recv()
            mid(b - 4)

        @pl.when(b >= 2)
        def _():
            ct_copy(b - 2).wait()

        @pl.when(b + TS - 2 < rows)
        def _():
            tok_copy(b + TS - 2).start()

        for k in range(2 * WS):
            @pl.when(b == 3 * k + 2)
            def _():
                (w2_copy if k % 2 else w1_copy)(k // 2).start()

        tok_copy(b).wait()
        sums(b - 1)
        gate(b)
        ct_copy(b).start()
        return 0

    lax.fori_loop(1, rows, step, 0)
    zc = z_copies()
    for z in zc:
        z.start()
    d_copy(rows - 2).start()
    x_copy(rows - 5).start()
    sums(rows - 1)
    d_copy(rows - 4).wait_recv()
    mid(rows - 4)
    d_copy(rows - 1).start()
    d_copy(rows - 3).wait_recv()
    mid(rows - 3)
    x_copy(rows - 4).start()
    d_copy(rows - 2).wait_recv()
    mid(rows - 2)
    x_copy(rows - 3).start()
    d_copy(rows - 1).wait_recv()
    mid(rows - 1)
    x_copy(rows - 2).start()
    ct_copy(rows - 2).wait()
    ct_copy(rows - 1).wait()
    for z in zc:
        z.wait_recv()
    x_copy(rows - 1).start()

    zs[...] = jnp.ones_like(zs)
    zs[:own, :] = zt[pl.ds(pl.multiple_of(me * own, own), own), :] + zr[0] + zr[1] + zr[2]
    zs[...] = 1.0 / zs[...].T

    swap = _swap_matrix()
    for h in range(rows // G):
        def wait_x(i, _):
            x_copy(i).wait_recv()
            return 0
        lax.fori_loop(h * G, (h + 1) * G, wait_x, 0)
        for g in range(own // G):
            near = rbuf[pl.ds(h * G, G), xi, pl.ds(g * G, G), :].reshape(G * G, width)
            far = qbuf[pl.ds(h * G, G), pl.ds(g * G, G), :].reshape(G * G, width)
            s = (jnp.dot(swap, near, preferred_element_type=jnp.float32)
                 + jnp.dot(swap, far, preferred_element_type=jnp.float32))
            for k in range(G):
                zinv = zs[h * G:(h + 1) * G, g * G + k:g * G + k + 1]
                xst[g * G + k, pl.ds(h * G, G), :] = (s[k * G:(k + 1) * G] * zinv).astype(jnp.bfloat16)

    def at(dev, e):
        return ys_hbm.at[pl.ds(dev * own + e * per, per)]

    def l_copy(e):
        return pltpu.make_async_copy(yst.at[e], at(me, e), l_sem.at[e])

    def c_copy(e):
        return remote(yst.at[e], at(me, e), c_ssem.at[e], c_rsem.at[e], core_peer)

    def p_copy(e):
        return remote(yst.at[e], at(me, e), p_ssem.at[e], p_rsem.at[e], x_peer)

    def f_copy(e):
        return remote(at(x_peer, e), at(x_peer, e), f_ssem.at[e], f_rsem.at[e], core_peer)

    def send(e):
        p_copy(e).start()
        c_copy(e).start()
        l_copy(e).start()

    def expert(e, _):
        @pl.when(e >= 1)
        def _():
            send(e - 1)

        @pl.when(e >= 4)
        def _():
            p_copy(e - 4).wait_recv()
            f_copy(e - 4).start()

        w1_copy(e).wait()
        w2_copy(e).wait()
        slot = e % WS
        xs = xst[pl.ds(e * per, per)].reshape(per * rows, width)
        acc = None
        for f in range(w1.shape[2] // FC):
            hid = jnp.dot(xs, w1[slot, :, f * FC:(f + 1) * FC], preferred_element_type=jnp.float32)
            hid = jax.nn.gelu(hid).astype(jnp.bfloat16)
            part = jnp.dot(hid, w2[slot, f * FC:(f + 1) * FC, :], preferred_element_type=jnp.float32)
            acc = part if acc is None else acc + part
        yst[e] = acc.astype(jnp.bfloat16).reshape(per, rows, width)

        @pl.when(e + WS < experts)
        def _():
            w1_copy(e + WS).start()
            w2_copy(e + WS).start()

        return 0

    lax.fori_loop(0, experts, expert, 0)

    def drain(b, _):
        d_copy(b).wait_send()
        x_copy(b).wait_send()
        return 0
    lax.fori_loop(0, rows, drain, 0)
    for z in zc:
        z.wait_send()
    send(experts - 1)
    for e in range(experts - 4, experts):
        p_copy(e).wait_recv()
        f_copy(e).start()

    def finish(e, _):
        l_copy(e).wait()
        c_copy(e).wait()
        p_copy(e).wait_send()
        f_copy(e).wait()
        return 0
    lax.fori_loop(0, experts, finish, 0)


def _combine_kernel(len_ref, ct_ref, ys_ref, y_ref, ysb):
    b = pl.program_id(0)
    toks, width = y_ref.shape[1], y_ref.shape[2]
    slots = ys_ref.shape[0]

    @pl.when(b % G == 0)
    def _():
        swap = _swap_matrix()
        for g in range(slots // G):
            blk = ys_ref[pl.ds(g * G, G)].reshape(G * G, width)
            out = jnp.dot(swap, blk, preferred_element_type=jnp.float32).astype(jnp.bfloat16)
            ysb[:, pl.ds(g * G, G), :] = out.reshape(G, G, width)

    limit = len_ref[b] - lax.axis_index("seq") * toks
    own = ysb[b % G]
    for k in range(toks // BLK):
        c = ct_ref[0, :, k * BLK:(k + 1) * BLK]
        mixed = lax.dot_general(c, own, (((0,), (0,)), ((), ())), preferred_element_type=jnp.float32)
        pos = lax.broadcasted_iota(jnp.int32, (BLK, 1), 0) + k * BLK
        y_ref[0, k * BLK:(k + 1) * BLK, :] = jnp.where(pos < limit, mixed, 0.0).astype(jnp.bfloat16)


def solution(mesh):
    def shard_body(tok_blk, len_blk, slot_params, logit_scale, w_in_blk, w_out_blk):
        rows, toks, width = tok_blk.shape
        slots = slot_params.shape[1]
        experts, _, ff = w_in_blk.shape
        own = slots // mesh.shape["seq"]
        per = own // experts
        bf, f32 = jnp.bfloat16, jnp.float32
        any_spec = pl.BlockSpec(memory_space=pl.ANY)
        smem = pl.BlockSpec(memory_space=pltpu.SMEM)
        dma = pltpu.SemaphoreType.DMA
        ys, ct = pl.pallas_call(
            functools.partial(_front_kernel, rows, experts),
            out_shape=(jax.ShapeDtypeStruct((slots, rows, width), bf),
                       jax.ShapeDtypeStruct((rows, slots, toks), bf)),
            in_specs=[smem, smem, pl.BlockSpec(memory_space=pltpu.VMEM), any_spec, any_spec, any_spec],
            out_specs=(any_spec, any_spec),
            scratch_shapes=[
                pltpu.VMEM((TS, toks, width), bf),
                pltpu.VMEM((slots, width), bf),
                pltpu.VMEM((slots, toks), bf),
                pltpu.VMEM((2, slots, toks), bf),
                pltpu.VMEM((rows, 2, 2, own, width), bf),
                pltpu.VMEM((rows, 2, own, width), bf),
                pltpu.VMEM((rows, own, width), bf),
                pltpu.VMEM((own, rows, width), bf),
                pltpu.VMEM((slots, 128), f32),
                pltpu.VMEM((3, own, 128), f32),
                pltpu.VMEM((128, 128), f32),
                pltpu.VMEM((experts, per, rows, width), bf),
                pltpu.VMEM((WS, width, ff), bf),
                pltpu.VMEM((WS, ff, width), bf),
                dma((TS,)), dma((2,)), dma((WS, 2)), dma((3,)), dma((3,)),
                dma((rows,)), dma((rows,)), dma((rows,)), dma((rows,)),
                dma((experts,)), dma((experts,)), dma((experts,)), dma((experts,)),
                dma((experts,)), dma((experts,)), dma((experts,)),
            ],
            compiler_params=pltpu.CompilerParams(
                collective_id=0, has_side_effects=True, vmem_limit_bytes=67_000_000),
            name="front",
        )(len_blk, logit_scale, slot_params, tok_blk, w_in_blk, w_out_blk)
        return pl.pallas_call(
            _combine_kernel,
            grid_spec=pltpu.PrefetchScalarGridSpec(
                num_scalar_prefetch=1,
                grid=(rows,),
                in_specs=[
                    pl.BlockSpec((1, slots, toks), lambda b, n: (b, 0, 0)),
                    pl.BlockSpec((slots, G, width), lambda b, n: (0, b // G, 0)),
                ],
                out_specs=pl.BlockSpec((1, toks, width), lambda b, n: (b, 0, 0)),
                scratch_shapes=[pltpu.VMEM((G, slots, width), bf)],
            ),
            out_shape=jax.ShapeDtypeStruct((rows, toks, width), bf),
            compiler_params=pltpu.CompilerParams(vmem_limit_bytes=60_000_000),
            name="combine",
        )(len_blk, ct, ys)

    return jax.shard_map(
        shard_body,
        mesh=mesh,
        in_specs=(P("data", "seq", None), P("data"), P(None, None), P(None), P("seq", None, None), P("seq", None, None)),
        out_specs=P("data", "seq", None),
        check_vma=False,
    )
```

```python
import functools

import jax
import jax.numpy as jnp
from jax import lax
from jax.experimental import pallas as pl
from jax.experimental.pallas import tpu as pltpu
from jax.sharding import PartitionSpec as P

BLK = 256
TS = 5
WS = 4
PARTS = 4
YS = 8
FC = 512
G = 16


def _swap_matrix():
    r = lax.broadcasted_iota(jnp.int32, (G * G, G * G), 0)
    c = lax.broadcasted_iota(jnp.int32, (G * G, G * G), 1)
    hit = ((r >> 4) == (c & 15)) & ((r & 15) == (c >> 4))
    return jnp.where(hit, 1.0, 0.0).astype(jnp.bfloat16)


def _front_kernel(rows, experts, len_ref, scale_ref, phi_hbm, x_hbm, win_hbm, wout_hbm,
                  ys_hbm, ct_hbm,
                  xbuf, phi_ref, phit, wt, ctst, sbuf, rbuf, qbuf, xst, zt, zr, zs, yst, w1, w2,
                  phi_sem, tok_sem, ct_sem, w_sem, z_ssem, z_rsem,
                  d_ssem, d_rsem, x_ssem, x_rsem,
                  l_sem, k_sem, c_ssem, c_rsem, p_ssem, p_rsem, f_ssem, f_rsem):
    toks, width = x_hbm.shape[1], x_hbm.shape[2]
    slots = phi_ref.shape[1]
    own = sbuf.shape[3]
    per = own // experts
    me = lax.axis_index("seq")
    xi = me // 2
    ci = me % 2
    core_peer = 2 * xi + (1 - ci)
    x_peer = 2 * (1 - xi) + ci
    diag = 2 * (1 - xi) + (1 - ci)

    def remote(src, dst, ssem, rsem, dev):
        return pltpu.make_async_remote_copy(
            src_ref=src, dst_ref=dst, send_sem=ssem, recv_sem=rsem,
            device_id={"seq": dev}, device_id_type=pl.DeviceIdType.MESH)

    def tok_copy(b):
        return pltpu.make_async_copy(x_hbm.at[b], xbuf.at[b % TS], tok_sem.at[b % TS])

    def ct_copy(b):
        return pltpu.make_async_copy(ctst.at[b % 2], ct_hbm.at[b], ct_sem.at[b % 2])

    def w1_copy(e):
        return pltpu.make_async_copy(win_hbm.at[e], w1.at[e % WS], w_sem.at[e % WS, 0])

    def w2_copy(e):
        return pltpu.make_async_copy(wout_hbm.at[e], w2.at[e % WS], w_sem.at[e % WS, 1])

    def w1_part(e, k):
        n = width // PARTS
        cut = pl.ds(pl.multiple_of(k * n, n), n)
        return pltpu.make_async_copy(win_hbm.at[e, cut], w1.at[e, cut], w_sem.at[e, 0])

    def w2_part(e, k):
        n = w2.shape[1] // PARTS
        cut = pl.ds(pl.multiple_of(k * n, n), n)
        return pltpu.make_async_copy(wout_hbm.at[e, cut], w2.at[e, cut], w_sem.at[e, 1])

    def d_copy(b):
        return remote(sbuf.at[b, :, 1 - ci], rbuf.at[b], d_ssem, d_rsem.at[b], core_peer)

    def x_copy(b):
        return remote(rbuf.at[b, 1 - xi], qbuf.at[b], x_ssem, x_rsem.at[b // G], x_peer)

    def z_copies():
        out = []
        for k, dev in enumerate((core_peer, x_peer, diag)):
            out.append(remote(zt.at[pl.ds(pl.multiple_of(dev * own, own), own)], zr.at[k],
                              z_ssem.at[k], z_rsem.at[k], dev))
        return out

    phi_copy = pltpu.make_async_copy(phi_hbm, phi_ref, phi_sem)
    phi_copy.start()
    for k in range(TS - 2):
        tok_copy(k).start()

    barrier = pltpu.get_barrier_semaphore()
    for dev in (core_peer, x_peer, diag):
        pl.semaphore_signal(barrier, inc=1, device_id={"seq": dev}, device_id_type=pl.DeviceIdType.MESH)

    phi_copy.wait()
    scale = scale_ref[0]
    phi = phi_ref[...].astype(jnp.float32)
    col_inv = lax.rsqrt(jnp.sum(phi * phi, axis=0, keepdims=True) + 1e-6)
    phit[...] = (phi * (scale * col_inv)).T.astype(jnp.bfloat16)
    zt[...] = jnp.zeros_like(zt)

    def gate(b):
        limit = len_ref[b] - me * toks
        zacc = None
        for k in range(toks // BLK):
            cols = pl.ds(k * BLK, BLK)
            xf = xbuf[b % TS, cols, :].astype(jnp.float32)
            inv = lax.rsqrt(jnp.sum(xf * xf, axis=1, keepdims=True) + 1e-6)
            xn = (xf * inv).astype(jnp.bfloat16)
            lt = lax.dot_general(phit[...], xn, (((1,), (1,)), ((), ())),
                                 preferred_element_type=jnp.float32)
            e = jnp.exp(lt - scale)
            den = jnp.sum(e, axis=0, keepdims=True)
            ctst[b % 2, :, cols] = (e * (1.0 / den)).astype(jnp.bfloat16)
            pos = lax.broadcasted_iota(jnp.int32, (1, BLK), 1) + k * BLK
            w = jnp.where(pos < limit, e, 0.0)
            wt[:, cols] = w.astype(jnp.bfloat16)
            for h in range(BLK // 128):
                part = w[:, h * 128:(h + 1) * 128]
                zacc = part if zacc is None else zacc + part
        zcol = jnp.sum(zacc, axis=1, keepdims=True)
        lane = lax.broadcasted_iota(jnp.int32, zt.shape, 1)
        zt[...] = jnp.where(lane == b, zcol, zt[...])

    def sums(b, slot):
        s = jnp.dot(wt[...], xbuf[slot], preferred_element_type=jnp.float32)
        sbuf[b] = s.astype(jnp.bfloat16).reshape(2, 2, own, width)

    def mid(b):
        for h in range(2):
            rbuf[b, h] = (rbuf[b, h].astype(jnp.float32)
                          + sbuf[b, h, ci].astype(jnp.float32)).astype(jnp.bfloat16)

    wt[...] = jnp.zeros_like(wt)
    pl.semaphore_wait(barrier, 3)

    def step(b, _):
        @pl.when(b >= 2)
        def _():
            d_copy(b - 2).start()
            ct_copy(b - 2).wait()

        @pl.when(b + TS - 2 < rows)
        def _():
            tok_copy(b + TS - 2).start()

        e, part = b // (2 * PARTS), b % PARTS

        @pl.when(b % (2 * PARTS) < PARTS)
        def _():
            w1_part(e, part).start()

        @pl.when(b % (2 * PARTS) >= PARTS)
        def _():
            w2_part(e, part).start()

        @pl.when(b >= 3)
        def _():
            d_copy(b - 3).wait_recv()
            mid(b - 3)

        tok_copy(b).wait()
        sums(jnp.maximum(b - 1, 0), (b + TS - 1) % TS)
        gate(b)
        ct_copy(b).start()

        @pl.when(b >= 3)
        def _():
            x_copy(b - 3).start()
        return 0

    lax.fori_loop(0, rows, step, 0)
    d_copy(rows - 2).start()
    zc = z_copies()
    for z in zc:
        z.start()
    sums(rows - 1, (rows - 1) % TS)
    d_copy(rows - 3).wait_recv()
    mid(rows - 3)
    d_copy(rows - 1).start()
    d_copy(rows - 2).wait_recv()
    mid(rows - 2)
    x_copy(rows - 3).start()
    d_copy(rows - 1).wait_recv()
    mid(rows - 1)
    x_copy(rows - 2).start()
    remote(rbuf, rbuf, d_ssem, d_rsem.at[0], core_peer).wait_send()
    ct_copy(rows - 2).wait()
    ct_copy(rows - 1).wait()
    x_copy(rows - 1).start()
    for z in zc:
        z.wait_recv()

    zs[...] = jnp.ones_like(zs)
    zs[:own, :] = zt[pl.ds(pl.multiple_of(me * own, own), own), :] + zr[0] + zr[1] + zr[2]
    zs[...] = 1.0 / zs[...].T

    swap = _swap_matrix()

    def settle(h, _):
        cut = pl.ds(pl.multiple_of(h * G, G), G)
        remote(qbuf.at[cut], qbuf.at[cut], x_ssem, x_rsem.at[h], x_peer).wait_recv()
        zi = zs[cut, :]
        for g in range(own // G):
            near = rbuf[cut, xi, pl.ds(g * G, G), :].reshape(G * G, width)
            far = qbuf[cut, pl.ds(g * G, G), :].reshape(G * G, width)
            s = (jnp.dot(swap, near, preferred_element_type=jnp.float32)
                 + jnp.dot(swap, far, preferred_element_type=jnp.float32))
            for k in range(G):
                zinv = zi[:, g * G + k:g * G + k + 1]
                xst[g * G + k, cut, :] = (s[k * G:(k + 1) * G] * zinv).astype(jnp.bfloat16)
        return 0

    lax.fori_loop(0, rows // G, settle, 0)

    def at(dev, e):
        return ys_hbm.at[pl.ds(dev * own + e * per, per)]

    def at_all(dev):
        return ys_hbm.at[pl.ds(dev * own, own)]

    def l_copy(e):
        return pltpu.make_async_copy(yst.at[e], at(me, e), l_sem)

    def c_copy(e):
        return remote(yst.at[e], at(me, e), c_ssem, c_rsem, core_peer)

    def p_copy(e):
        return remote(yst.at[e], sbuf.at[e, 0], p_ssem, p_rsem.at[e], x_peer)

    def f_copy(e):
        return remote(sbuf.at[e, 0], at(x_peer, e), f_ssem, f_rsem, core_peer)

    def k_copy(e):
        return pltpu.make_async_copy(sbuf.at[e, 0], at(x_peer, e), k_sem)

    def send(e):
        p_copy(e).start()
        c_copy(e).start()
        l_copy(e).start()

    def forward(e):
        p_copy(e).wait_recv()
        f_copy(e).start()
        k_copy(e).start()

    def expert(e, _):
        @pl.when(e >= 1)
        def _():
            send(e - 1)

        @pl.when(e >= 4)
        def _():
            forward(e - 4)

        w1_copy(e).wait()
        w2_copy(e).wait()
        slot = e % WS
        xs = xst[pl.ds(e * per, per)].reshape(per * rows, width)
        acc = None
        for f in range(w1.shape[2] // FC):
            hid = jnp.dot(xs, w1[slot, :, f * FC:(f + 1) * FC], preferred_element_type=jnp.float32)
            hid = jax.nn.gelu(hid).astype(jnp.bfloat16)
            part = jnp.dot(hid, w2[slot, f * FC:(f + 1) * FC, :], preferred_element_type=jnp.float32)
            acc = part if acc is None else acc + part
        yst[e] = acc.astype(jnp.bfloat16).reshape(per, rows, width)

        @pl.when(e + WS < experts)
        def _():
            w1_copy(e + WS).start()
            w2_copy(e + WS).start()

        return 0

    lax.fori_loop(0, experts, expert, 0)

    send(experts - 1)
    for e in range(experts - 4, experts):
        forward(e)
    remote(qbuf, qbuf, x_ssem, x_rsem.at[0], x_peer).wait_send()
    for z in zc:
        z.wait_send()
    mine, theirs = at_all(me), at_all(x_peer)
    remote(xst, mine, c_ssem, c_rsem, core_peer).wait()
    remote(xst, mine, p_ssem, p_rsem.at[0], x_peer).wait_send()
    remote(xst, theirs, f_ssem, f_rsem, core_peer).wait()
    pltpu.make_async_copy(xst, mine, l_sem).wait()
    pltpu.make_async_copy(xst, theirs, k_sem).wait()


def _combine_kernel(len_ref, ct_hbm, ys_hbm, y_hbm, ysv, ysb, ctb, yb, ys_sem, ct_sem, y_sem):
    rows, toks, width = y_hbm.shape
    slots = ys_hbm.shape[0]
    start = lax.axis_index("seq") * toks

    def ys_copy(h):
        return pltpu.make_async_copy(ys_hbm.at[:, pl.ds(pl.multiple_of(h * G, G), G)], ysv.at[h], ys_sem.at[h])

    def ct_copy(b):
        return pltpu.make_async_copy(ct_hbm.at[b], ctb.at[b % YS], ct_sem.at[b % YS])

    def y_copy(b):
        return pltpu.make_async_copy(yb.at[b % YS], y_hbm.at[b], y_sem.at[b % YS])

    ys_copy(0).start()
    for k in range(YS - 1):
        ct_copy(k).start()
    for h in range(1, rows // G):
        ys_copy(h).start()
    swap = _swap_matrix()

    def half(h, _):
        ys_copy(h).wait()
        for g in range(slots // G):
            blk = ysv[h, pl.ds(g * G, G)].reshape(G * G, width)
            out = jnp.dot(swap, blk, preferred_element_type=jnp.float32).astype(jnp.bfloat16)
            ysb[:, pl.ds(g * G, G), :] = out.reshape(G, G, width)

        def row(i, _):
            b = h * G + i

            @pl.when(b + YS - 1 < rows)
            def _():
                ct_copy(b + YS - 1).start()

            ct_copy(b).wait()

            @pl.when(b >= YS)
            def _():
                y_copy(b - YS).wait()

            limit = len_ref[b] - start

            @pl.when(limit > 0)
            def _():
                for k in range(toks // BLK):
                    c = ctb[b % YS, :, k * BLK:(k + 1) * BLK]
                    mixed = lax.dot_general(c, ysb[i], (((0,), (0,)), ((), ())),
                                            preferred_element_type=jnp.float32)
                    pos = lax.broadcasted_iota(jnp.int32, (BLK, 1), 0) + k * BLK
                    yb[b % YS, k * BLK:(k + 1) * BLK, :] = jnp.where(pos < limit, mixed, 0.0).astype(jnp.bfloat16)

            @pl.when(limit <= 0)
            def _():
                yb[b % YS] = jnp.zeros((toks, width), jnp.bfloat16)

            y_copy(b).start()
            return 0

        lax.fori_loop(0, G, row, 0)
        return 0

    lax.fori_loop(0, rows // G, half, 0)

    def finish(b, _):
        y_copy(b).wait()
        return 0
    lax.fori_loop(rows - YS, rows, finish, 0)


def solution(mesh):
    def shard_body(tok_blk, len_blk, slot_params, logit_scale, w_in_blk, w_out_blk):
        rows, toks, width = tok_blk.shape
        slots = slot_params.shape[1]
        experts, _, ff = w_in_blk.shape
        own = slots // mesh.shape["seq"]
        per = own // experts
        bf, f32 = jnp.bfloat16, jnp.float32
        any_spec = pl.BlockSpec(memory_space=pl.ANY)
        smem = pl.BlockSpec(memory_space=pltpu.SMEM)
        dma = pltpu.SemaphoreType.DMA
        ys, ct = pl.pallas_call(
            functools.partial(_front_kernel, rows, experts),
            out_shape=(jax.ShapeDtypeStruct((slots, rows, width), bf),
                       jax.ShapeDtypeStruct((rows, slots, toks), bf)),
            in_specs=[smem, smem, any_spec, any_spec, any_spec, any_spec],
            out_specs=(any_spec, any_spec),
            scratch_shapes=[
                pltpu.VMEM((TS, toks, width), bf),
                pltpu.VMEM((width, slots), bf),
                pltpu.VMEM((slots, width), bf),
                pltpu.VMEM((slots, toks), bf),
                pltpu.VMEM((2, slots, toks), bf),
                pltpu.VMEM((rows, 2, 2, own, width), bf),
                pltpu.VMEM((rows, 2, own, width), bf),
                pltpu.VMEM((rows, own, width), bf),
                pltpu.VMEM((own, rows, width), bf),
                pltpu.VMEM((slots, 128), f32),
                pltpu.VMEM((3, own, 128), f32),
                pltpu.VMEM((128, 128), f32),
                pltpu.VMEM((experts, per, rows, width), bf),
                pltpu.VMEM((WS, width, ff), bf),
                pltpu.VMEM((WS, ff, width), bf),
                dma, dma((TS,)), dma((2,)), dma((WS, 2)), dma((3,)), dma((3,)),
                dma, dma((rows,)), dma, dma((rows // G,)),
                dma, dma, dma, dma, dma, dma((experts,)), dma, dma,
            ],
            compiler_params=pltpu.CompilerParams(
                collective_id=0, has_side_effects=True, vmem_limit_bytes=67_000_000),
            name="front",
        )(len_blk, logit_scale, slot_params, tok_blk, w_in_blk, w_out_blk)
        return pl.pallas_call(
            _combine_kernel,
            in_specs=[smem, any_spec, any_spec],
            out_specs=any_spec,
            out_shape=jax.ShapeDtypeStruct((rows, toks, width), bf),
            scratch_shapes=[
                pltpu.VMEM((rows // G, slots, G, width), bf),
                pltpu.VMEM((G, slots, width), bf),
                pltpu.VMEM((YS, slots, toks), bf),
                pltpu.VMEM((YS, toks, width), bf),
                dma((rows // G,)), dma((YS,)), dma((YS,)),
            ],
            compiler_params=pltpu.CompilerParams(vmem_limit_bytes=60_000_000),
            name="combine",
        )(len_blk, ct, ys)

    return jax.shard_map(
        shard_body,
        mesh=mesh,
        in_specs=(P("data", "seq", None), P("data"), P(None, None), P(None), P("seq", None, None), P("seq", None, None)),
        out_specs=P("data", "seq", None),
        check_vma=False,
    )
```

```python
import functools

import jax
import jax.numpy as jnp
from jax import lax
from jax.experimental import pallas as pl
from jax.experimental.pallas import tpu as pltpu
from jax.sharding import PartitionSpec as P

BLK = 256
TS = 4
SS = 8
WS = 14
FC = 1024
FS = 1024
LAG = 3
YS = 8
G = 16


def _swap_matrix():
    r = lax.broadcasted_iota(jnp.int32, (G * G, G * G), 0)
    c = lax.broadcasted_iota(jnp.int32, (G * G, G * G), 1)
    hit = ((r >> 4) == (c & 15)) & ((r & 15) == (c >> 4))
    return jnp.where(hit, 1.0, 0.0).astype(jnp.bfloat16)


def _front_kernel(rows, experts, len_ref, scale_ref, phi_hbm, x_hbm, win_hbm, wout_hbm,
                  ys_hbm, ct_hbm,
                  xbuf, phi_ref, phit, wt, ctst, sbuf, rbuf, qbuf, xst, zt, zr, zs, w1, w2,
                  phi_sem, tok_sem, ct_sem, w_sem, z_ssem, z_rsem,
                  d_ssem, d_rsem, x_ssem, x_rsem,
                  l_sem, k_sem, c_ssem, c_rsem, p_ssem, p_rsem, f_ssem, f_rsem):
    toks, width = x_hbm.shape[1], x_hbm.shape[2]
    slots = phi_ref.shape[1]
    own = sbuf.shape[3]
    per = own // experts
    units = win_hbm.shape[2] // FC
    many = per * rows
    me = lax.axis_index("seq")
    xi = me // 2
    ci = me % 2
    core_peer = 2 * xi + (1 - ci)
    x_peer = 2 * (1 - xi) + ci
    diag = 2 * (1 - xi) + (1 - ci)

    def remote(src, dst, ssem, rsem, dev):
        return pltpu.make_async_remote_copy(
            src_ref=src, dst_ref=dst, send_sem=ssem, recv_sem=rsem,
            device_id={"seq": dev}, device_id_type=pl.DeviceIdType.MESH)

    def tok_copy(b):
        return pltpu.make_async_copy(x_hbm.at[b], xbuf.at[b % TS], tok_sem.at[b % TS])

    def ct_copy(b):
        return pltpu.make_async_copy(ctst.at[b % 2], ct_hbm.at[b], ct_sem.at[b % 2])

    def w1_copy(u):
        cols = pl.ds(pl.multiple_of(u % units * FC, FC), FC)
        return pltpu.make_async_copy(win_hbm.at[u // units, :, cols], w1.at[u % WS], w_sem.at[u % WS, 0])

    def w2_copy(u):
        cut = pl.ds(pl.multiple_of(u % units * FC, FC), FC)
        return pltpu.make_async_copy(wout_hbm.at[u // units, cut], w2.at[u % WS], w_sem.at[u % WS, 1])

    def d_copy(b):
        return remote(sbuf.at[b % SS, :, 1 - ci], rbuf.at[b], d_ssem.at[b % SS], d_rsem.at[b], core_peer)

    def x_copy(b):
        return remote(rbuf.at[b, 1 - xi], qbuf.at[b], x_ssem, x_rsem.at[b // G], x_peer)

    def z_copies():
        out = []
        for k, dev in enumerate((core_peer, x_peer, diag)):
            out.append(remote(zt.at[pl.ds(pl.multiple_of(dev * own, own), own)], zr.at[k],
                              z_ssem.at[k], z_rsem.at[k], dev))
        return out

    phi_copy = pltpu.make_async_copy(phi_hbm, phi_ref, phi_sem)
    phi_copy.start()
    for k in range(TS - 2):
        tok_copy(k).start()

    barrier = pltpu.get_barrier_semaphore()
    for dev in (core_peer, x_peer, diag):
        pl.semaphore_signal(barrier, inc=1, device_id={"seq": dev}, device_id_type=pl.DeviceIdType.MESH)

    phi_copy.wait()
    scale = scale_ref[0]
    phi = phi_ref[...].astype(jnp.float32)
    col_inv = lax.rsqrt(jnp.sum(phi * phi, axis=0, keepdims=True) + 1e-6)
    phit[...] = (phi * (scale * col_inv)).T.astype(jnp.bfloat16)
    zt[...] = jnp.zeros_like(zt)

    def gate(b):
        limit = len_ref[b] - me * toks
        zacc = None
        for k in range(toks // BLK):
            cols = pl.ds(k * BLK, BLK)
            xf = xbuf[b % TS, cols, :].astype(jnp.float32)
            inv = lax.rsqrt(jnp.sum(xf * xf, axis=1, keepdims=True) + 1e-6)
            xn = (xf * inv).astype(jnp.bfloat16)
            lt = lax.dot_general(phit[...], xn, (((1,), (1,)), ((), ())),
                                 preferred_element_type=jnp.float32)
            e = jnp.exp(lt - scale)
            den = jnp.sum(e, axis=0, keepdims=True)
            ctst[b % 2, :, cols] = (e * (1.0 / den)).astype(jnp.bfloat16)
            pos = lax.broadcasted_iota(jnp.int32, (1, BLK), 1) + k * BLK
            w = jnp.where(pos < limit, e, 0.0)
            wt[:, cols] = w.astype(jnp.bfloat16)
            for h in range(BLK // 128):
                part = w[:, h * 128:(h + 1) * 128]
                zacc = part if zacc is None else zacc + part
        zcol = jnp.sum(zacc, axis=1, keepdims=True)
        lane = lax.broadcasted_iota(jnp.int32, zt.shape, 1)
        zt[...] = jnp.where(lane == b, zcol, zt[...])

    def sums(b, slot):
        s = jnp.dot(wt[...], xbuf[slot], preferred_element_type=jnp.float32)
        sbuf[b % SS] = s.astype(jnp.bfloat16).reshape(2, 2, own, width)

    def mid(b):
        for h in range(2):
            rbuf[b, h] = (rbuf[b, h].astype(jnp.float32)
                          + sbuf[b % SS, h, ci].astype(jnp.float32)).astype(jnp.bfloat16)

    wt[...] = jnp.zeros_like(wt)
    pl.semaphore_wait(barrier, 3)

    def step(b, _):
        @pl.when(b >= 2)
        def _():
            d_copy(b - 2).start()
            ct_copy(b - 2).wait()

        @pl.when(b + TS - 2 < rows)
        def _():
            tok_copy(b + TS - 2).start()

        @pl.when((b < 2 * WS) & (b % 2 == 0))
        def _():
            w1_copy(b // 2).start()

        @pl.when((b < 2 * WS) & (b % 2 == 1))
        def _():
            w2_copy(b // 2).start()

        @pl.when(b > SS)
        def _():
            d_copy(b - 1 - SS).wait_send()

        @pl.when(b >= 3)
        def _():
            d_copy(b - 3).wait_recv()
            mid(b - 3)

        tok_copy(b).wait()
        sums(jnp.maximum(b - 1, 0), (b + TS - 1) % TS)
        gate(b)
        ct_copy(b).start()

        @pl.when(b >= 3)
        def _():
            x_copy(b - 3).start()
        return 0

    lax.fori_loop(0, rows, step, 0)
    d_copy(rows - 2).start()
    zc = z_copies()
    for z in zc:
        z.start()
    d_copy(rows - 1 - SS).wait_send()
    sums(rows - 1, (rows - 1) % TS)
    d_copy(rows - 3).wait_recv()
    mid(rows - 3)
    d_copy(rows - 1).start()
    d_copy(rows - 2).wait_recv()
    mid(rows - 2)
    x_copy(rows - 3).start()
    d_copy(rows - 1).wait_recv()
    mid(rows - 1)
    x_copy(rows - 2).start()
    ct_copy(rows - 2).wait()
    ct_copy(rows - 1).wait()
    x_copy(rows - 1).start()
    for z in zc:
        z.wait_recv()

    zs[...] = jnp.ones_like(zs)
    zs[:own, :] = zt[pl.ds(pl.multiple_of(me * own, own), own), :] + zr[0] + zr[1] + zr[2]
    zs[...] = 1.0 / zs[...].T

    swap = _swap_matrix()

    def settle(h, _):
        cut = pl.ds(pl.multiple_of(h * G, G), G)
        remote(qbuf.at[cut], qbuf.at[cut], x_ssem, x_rsem.at[h], x_peer).wait_recv()
        zi = zs[cut, :]
        for g in range(own // G):
            near = rbuf[cut, xi, pl.ds(g * G, G), :].reshape(G * G, width)
            far = qbuf[cut, pl.ds(g * G, G), :].reshape(G * G, width)
            s = (jnp.dot(swap, near, preferred_element_type=jnp.float32)
                 + jnp.dot(swap, far, preferred_element_type=jnp.float32))
            for k in range(G):
                zinv = zi[:, g * G + k:g * G + k + 1]
                xst[g * G + k, cut, :] = (s[k * G:(k + 1) * G] * zinv).astype(jnp.bfloat16)
        return 0

    lax.fori_loop(0, rows // G, settle, 0)

    for b in range(rows - SS, rows):
        d_copy(b).wait_send()

    def at(dev, e):
        return ys_hbm.at[pl.ds(pl.multiple_of((dev * experts + e) * many, many), many)]

    def at_all(dev):
        return ys_hbm.at[pl.ds(pl.multiple_of(dev * experts * many, many), experts * many)]

    def here(slot, e):
        return xbuf.at[slot, pl.ds(pl.multiple_of(e * many, many), many)]

    def l_copy(e):
        return pltpu.make_async_copy(here(0, e), at(me, e), l_sem)

    def c_copy(e):
        return remote(here(0, e), at(me, e), c_ssem, c_rsem, core_peer)

    def p_copy(e):
        return remote(here(0, e), here(1, e), p_ssem, p_rsem.at[e], x_peer)

    def f_copy(e):
        return remote(here(1, e), at(x_peer, e), f_ssem, f_rsem, core_peer)

    def k_copy(e):
        return pltpu.make_async_copy(here(1, e), at(x_peer, e), k_sem)

    def send(e):
        p_copy(e).start()
        c_copy(e).start()
        l_copy(e).start()

    def forward(e):
        p_copy(e).wait_recv()
        f_copy(e).start()
        k_copy(e).start()

    def expert(e, _):
        @pl.when(e >= 1)
        def _():
            send(e - 1)

        @pl.when(e >= LAG)
        def _():
            forward(e - LAG)

        xs = xst[pl.ds(e * per, per)].reshape(many, width)
        acc = None
        for f in range(units):
            u = e * units + f
            slot = u % WS
            w1_copy(u).wait()
            w2_copy(u).wait()
            for k in range(FC // FS):
                cut = slice(k * FS, (k + 1) * FS)
                hid = jnp.dot(xs, w1[slot, :, cut], preferred_element_type=jnp.float32)
                hid = jax.nn.gelu(hid).astype(jnp.bfloat16)
                part = jnp.dot(hid, w2[slot, cut, :], preferred_element_type=jnp.float32)
                acc = part if acc is None else acc + part

            @pl.when(u + WS < experts * units)
            def _():
                w1_copy(u + WS).start()
                w2_copy(u + WS).start()

        xbuf[0, pl.ds(pl.multiple_of(e * many, many), many)] = acc.astype(jnp.bfloat16)
        return 0

    lax.fori_loop(0, experts, expert, 0)
    send(experts - 1)
    for e in range(experts - LAG, experts):
        forward(e)
    remote(qbuf, qbuf, x_ssem, x_rsem.at[0], x_peer).wait_send()
    for z in zc:
        z.wait_send()
    mine, theirs, whole = at_all(me), at_all(x_peer), xbuf.at[0]
    remote(whole, mine, c_ssem, c_rsem, core_peer).wait()
    remote(whole, mine, p_ssem, p_rsem.at[0], x_peer).wait_send()
    remote(whole, theirs, f_ssem, f_rsem, core_peer).wait()
    pltpu.make_async_copy(whole, mine, l_sem).wait()
    pltpu.make_async_copy(whole, theirs, k_sem).wait()


def _combine_kernel(len_ref, ct_hbm, ys_hbm, y_hbm, ysv, ysb, ctb, yb, ys_sem, ct_sem, y_sem):
    rows, toks, width = y_hbm.shape
    slots = ys_hbm.shape[0]
    start = lax.axis_index("seq") * toks

    def ys_copy(h):
        return pltpu.make_async_copy(ys_hbm.at[:, pl.ds(pl.multiple_of(h * G, G), G)], ysv.at[h], ys_sem.at[h])

    def ct_copy(b):
        return pltpu.make_async_copy(ct_hbm.at[b], ctb.at[b % YS], ct_sem.at[b % YS])

    def y_copy(b):
        return pltpu.make_async_copy(yb.at[b % YS], y_hbm.at[b], y_sem.at[b % YS])

    ys_copy(0).start()
    for k in range(YS - 2):
        ct_copy(k).start()
    for h in range(1, rows // G):
        ys_copy(h).start()
    swap = _swap_matrix()

    def half(h, _):
        ys_copy(h).wait()
        for g in range(slots // G):
            blk = ysv[h, pl.ds(g * G, G)].reshape(G * G, width)
            out = jnp.dot(swap, blk, preferred_element_type=jnp.float32).astype(jnp.bfloat16)
            ysb[:, pl.ds(g * G, G), :] = out.reshape(G, G, width)

        def pair(p, _):
            first = h * G + 2 * p
            limits = []
            for j in range(2):
                b = first + j

                @pl.when(b + YS - 2 < rows)
                def _():
                    ct_copy(b + YS - 2).start()

                ct_copy(b).wait()

                @pl.when(b >= YS)
                def _():
                    y_copy(b - YS).wait()

                limits.append(len_ref[b] - start)

            @pl.when(jnp.maximum(limits[0], limits[1]) > 0)
            def _():
                for j in range(2):
                    slot = (first + j) % YS
                    own = ysb[2 * p + j]
                    for k in range(toks // BLK):
                        c = ctb[slot, :, k * BLK:(k + 1) * BLK]
                        mixed = lax.dot_general(c, own, (((0,), (0,)), ((), ())),
                                                preferred_element_type=jnp.float32)
                        pos = lax.broadcasted_iota(jnp.int32, (BLK, 1), 0) + k * BLK
                        yb[slot, k * BLK:(k + 1) * BLK, :] = jnp.where(
                            pos < limits[j], mixed, 0.0).astype(jnp.bfloat16)

            @pl.when(jnp.maximum(limits[0], limits[1]) <= 0)
            def _():
                for j in range(2):
                    yb[(first + j) % YS] = jnp.zeros((toks, width), jnp.bfloat16)

            for j in range(2):
                y_copy(first + j).start()
            return 0

        lax.fori_loop(0, G // 2, pair, 0)
        return 0

    lax.fori_loop(0, rows // G, half, 0)

    def finish(b, _):
        y_copy(b).wait()
        return 0
    lax.fori_loop(rows - YS, rows, finish, 0)


def solution(mesh):
    def shard_body(tok_blk, len_blk, slot_params, logit_scale, w_in_blk, w_out_blk):
        rows, toks, width = tok_blk.shape
        slots = slot_params.shape[1]
        experts, _, ff = w_in_blk.shape
        own = slots // mesh.shape["seq"]
        per = own // experts
        bf, f32 = jnp.bfloat16, jnp.float32
        any_spec = pl.BlockSpec(memory_space=pl.ANY)
        smem = pl.BlockSpec(memory_space=pltpu.SMEM)
        dma = pltpu.SemaphoreType.DMA
        ys, ct = pl.pallas_call(
            functools.partial(_front_kernel, rows, experts),
            out_shape=(jax.ShapeDtypeStruct((slots * rows, width), bf),
                       jax.ShapeDtypeStruct((rows, slots, toks), bf)),
            in_specs=[smem, smem, any_spec, any_spec, any_spec, any_spec],
            out_specs=(any_spec, any_spec),
            scratch_shapes=[
                pltpu.VMEM((TS, toks, width), bf),
                pltpu.VMEM((width, slots), bf),
                pltpu.VMEM((slots, width), bf),
                pltpu.VMEM((slots, toks), bf),
                pltpu.VMEM((2, slots, toks), bf),
                pltpu.VMEM((SS, 2, 2, own, width), bf),
                pltpu.VMEM((rows, 2, own, width), bf),
                pltpu.VMEM((rows, own, width), bf),
                pltpu.VMEM((own, rows, width), bf),
                pltpu.VMEM((slots, 128), f32),
                pltpu.VMEM((3, own, 128), f32),
                pltpu.VMEM((128, 128), f32),
                pltpu.VMEM((WS, width, FC), bf),
                pltpu.VMEM((WS, FC, width), bf),
                dma, dma((TS,)), dma((2,)), dma((WS, 2)), dma((3,)), dma((3,)),
                dma((SS,)), dma((rows,)), dma, dma((rows // G,)),
                dma, dma, dma, dma, dma, dma((experts,)), dma, dma,
            ],
            compiler_params=pltpu.CompilerParams(
                collective_id=0, has_side_effects=True, vmem_limit_bytes=67_000_000),
            name="front",
        )(len_blk, logit_scale, slot_params, tok_blk, w_in_blk, w_out_blk)
        return pl.pallas_call(
            _combine_kernel,
            in_specs=[smem, any_spec, any_spec],
            out_specs=any_spec,
            out_shape=jax.ShapeDtypeStruct((rows, toks, width), bf),
            scratch_shapes=[
                pltpu.VMEM((rows // G, slots, G, width), bf),
                pltpu.VMEM((G, slots, width), bf),
                pltpu.VMEM((YS, slots, toks), bf),
                pltpu.VMEM((YS, toks, width), bf),
                dma((rows // G,)), dma((YS,)), dma((YS,)),
            ],
            compiler_params=pltpu.CompilerParams(vmem_limit_bytes=60_000_000),
            name="combine",
        )(len_blk, ct, ys.reshape(slots, rows, width))

    return jax.shard_map(
        shard_body,
        mesh=mesh,
        in_specs=(P("data", "seq", None), P("data"), P(None, None), P(None), P("seq", None, None), P("seq", None, None)),
        out_specs=P("data", "seq", None),
        check_vma=False,
    )
```

```python
import functools

import jax
import jax.numpy as jnp
from jax import lax
from jax.experimental import pallas as pl
from jax.experimental.pallas import tpu as pltpu
from jax.sharding import PartitionSpec as P

BLK = 256
TS = 4
SS = 8
WS = 12
FC = 1024
FS = 1024
LAG = 3
YS = 8
G = 16


def _swap_matrix():
    r = lax.broadcasted_iota(jnp.int32, (G * G, G * G), 0)
    c = lax.broadcasted_iota(jnp.int32, (G * G, G * G), 1)
    hit = ((r >> 4) == (c & 15)) & ((r & 15) == (c >> 4))
    return jnp.where(hit, 1.0, 0.0).astype(jnp.bfloat16)


def _front_kernel(rows, experts, len_ref, scale_ref, phi_hbm, x_hbm, win_hbm, wout_hbm,
                  ys_hbm, ct_hbm,
                  xbuf, phi_ref, phit, wt, ctst, sbuf, rbuf, qbuf, xst, zt, zr, zs, w1, w2,
                  phi_sem, tok_sem, ct_sem, w_sem, z_ssem, z_rsem,
                  d_ssem, d_rsem, x_ssem, x_rsem,
                  l_sem, k_sem, c_ssem, c_rsem, p_ssem, p_rsem, f_ssem, f_rsem):
    toks, width = x_hbm.shape[1], x_hbm.shape[2]
    slots = phi_ref.shape[1]
    own = sbuf.shape[3]
    per = own // experts
    units = win_hbm.shape[2] // FC
    many = per * rows
    me = lax.axis_index("seq")
    xi = me // 2
    ci = me % 2
    core_peer = 2 * xi + (1 - ci)
    x_peer = 2 * (1 - xi) + ci
    diag = 2 * (1 - xi) + (1 - ci)

    def remote(src, dst, ssem, rsem, dev):
        return pltpu.make_async_remote_copy(
            src_ref=src, dst_ref=dst, send_sem=ssem, recv_sem=rsem,
            device_id={"seq": dev}, device_id_type=pl.DeviceIdType.MESH)

    def tok_copy(b):
        return pltpu.make_async_copy(x_hbm.at[b], xbuf.at[b % TS], tok_sem.at[b % TS])

    def ct_copy(b):
        return pltpu.make_async_copy(ctst.at[b % 2], ct_hbm.at[b], ct_sem.at[b % 2])

    def w1_copy(u):
        cols = pl.ds(pl.multiple_of(u % units * FC, FC), FC)
        return pltpu.make_async_copy(win_hbm.at[u // units, :, cols], w1.at[u % WS], w_sem.at[u % WS, 0])

    def w2_copy(u):
        cut = pl.ds(pl.multiple_of(u % units * FC, FC), FC)
        return pltpu.make_async_copy(wout_hbm.at[u // units, cut], w2.at[u % WS], w_sem.at[u % WS, 1])

    def d_copy(b):
        return remote(sbuf.at[b % SS, :, 1 - ci], rbuf.at[b], d_ssem.at[b % SS], d_rsem.at[b], core_peer)

    def x_copy(b):
        return remote(rbuf.at[b, 1 - xi], qbuf.at[b], x_ssem, x_rsem.at[b // G], x_peer)

    def z_copies():
        out = []
        for k, dev in enumerate((core_peer, x_peer, diag)):
            out.append(remote(zt.at[pl.ds(pl.multiple_of(dev * own, own), own)], zr.at[k],
                              z_ssem.at[k], z_rsem.at[k], dev))
        return out

    phi_copy = pltpu.make_async_copy(phi_hbm, phi_ref, phi_sem)
    phi_copy.start()
    for k in range(TS - 2):
        tok_copy(k).start()

    barrier = pltpu.get_barrier_semaphore()
    for dev in (core_peer, x_peer, diag):
        pl.semaphore_signal(barrier, inc=1, device_id={"seq": dev}, device_id_type=pl.DeviceIdType.MESH)

    phi_copy.wait()
    scale = scale_ref[0]
    phi = phi_ref[...].astype(jnp.float32)
    col_inv = lax.rsqrt(jnp.sum(phi * phi, axis=0, keepdims=True) + 1e-6)
    phit[...] = (phi * (scale * col_inv)).T.astype(jnp.bfloat16)
    zt[...] = jnp.zeros_like(zt)

    def gate(b):
        limit = len_ref[b] - me * toks
        zacc = None
        for k in range(toks // BLK):
            cols = pl.ds(k * BLK, BLK)
            xf = xbuf[b % TS, cols, :].astype(jnp.float32)
            inv = lax.rsqrt(jnp.sum(xf * xf, axis=1, keepdims=True) + 1e-6)
            xn = (xf * inv).astype(jnp.bfloat16)
            lt = lax.dot_general(phit[...], xn, (((1,), (1,)), ((), ())),
                                 preferred_element_type=jnp.float32)
            e = jnp.exp(lt - scale)
            den = jnp.sum(e, axis=0, keepdims=True)
            ctst[b % 2, :, cols] = (e * (1.0 / den)).astype(jnp.bfloat16)
            pos = lax.broadcasted_iota(jnp.int32, (1, BLK), 1) + k * BLK
            w = jnp.where(pos < limit, e, 0.0)
            wt[:, cols] = w.astype(jnp.bfloat16)
            for h in range(BLK // 128):
                part = w[:, h * 128:(h + 1) * 128]
                zacc = part if zacc is None else zacc + part
        zcol = jnp.sum(zacc, axis=1, keepdims=True)
        lane = lax.broadcasted_iota(jnp.int32, zt.shape, 1)
        zt[...] = jnp.where(lane == b, zcol, zt[...])

    def sums(b, slot):
        s = jnp.dot(wt[...], xbuf[slot], preferred_element_type=jnp.float32)
        sbuf[b % SS] = s.astype(jnp.bfloat16).reshape(2, 2, own, width)

    def mid(b):
        for h in range(2):
            rbuf[b, h] = (rbuf[b, h].astype(jnp.float32)
                          + sbuf[b % SS, h, ci].astype(jnp.float32)).astype(jnp.bfloat16)

    wt[...] = jnp.zeros_like(wt)
    pl.semaphore_wait(barrier, 3)

    def step(b, _):
        @pl.when(b >= 3)
        def _():
            x_copy(b - 3).start()

        @pl.when(b >= 2)
        def _():
            ct_copy(b - 2).wait()

        @pl.when(b + TS - 2 < rows)
        def _():
            tok_copy(b + TS - 2).start()

        @pl.when((b < 2 * WS) & (b % 2 == 0))
        def _():
            w1_copy(b // 2).start()

        @pl.when((b < 2 * WS) & (b % 2 == 1))
        def _():
            w2_copy(b // 2).start()

        @pl.when(b > SS)
        def _():
            d_copy(b - 1 - SS).wait_send()

        tok_copy(b).wait()
        sums(jnp.maximum(b - 1, 0), (b + TS - 1) % TS)
        gate(b)
        ct_copy(b).start()

        @pl.when(b >= 1)
        def _():
            d_copy(b - 1).start()

        @pl.when(b >= 2)
        def _():
            d_copy(b - 2).wait_recv()
            mid(b - 2)
        return 0

    lax.fori_loop(0, rows, step, 0)
    x_copy(rows - 3).start()
    zc = z_copies()
    for z in zc:
        z.start()
    d_copy(rows - 1 - SS).wait_send()
    sums(rows - 1, (rows - 1) % TS)
    d_copy(rows - 2).wait_recv()
    mid(rows - 2)
    d_copy(rows - 1).start()
    x_copy(rows - 2).start()
    d_copy(rows - 1).wait_recv()
    mid(rows - 1)
    ct_copy(rows - 2).wait()
    ct_copy(rows - 1).wait()
    x_copy(rows - 1).start()
    for z in zc:
        z.wait_recv()

    zs[...] = jnp.ones_like(zs)
    zs[:own, :] = zt[pl.ds(pl.multiple_of(me * own, own), own), :] + zr[0] + zr[1] + zr[2]
    zs[...] = 1.0 / zs[...].T

    swap = _swap_matrix()

    def settle(h, _):
        cut = pl.ds(pl.multiple_of(h * G, G), G)
        remote(qbuf.at[cut], qbuf.at[cut], x_ssem, x_rsem.at[h], x_peer).wait_recv()
        zi = zs[cut, :]
        for g in range(own // G):
            near = rbuf[cut, xi, pl.ds(g * G, G), :].reshape(G * G, width)
            far = qbuf[cut, pl.ds(g * G, G), :].reshape(G * G, width)
            s = (jnp.dot(swap, near, preferred_element_type=jnp.float32)
                 + jnp.dot(swap, far, preferred_element_type=jnp.float32))
            for k in range(G):
                zinv = zi[:, g * G + k:g * G + k + 1]
                xst[g * G + k, cut, :] = (s[k * G:(k + 1) * G] * zinv).astype(jnp.bfloat16)
        return 0

    lax.fori_loop(0, rows // G, settle, 0)

    for b in range(rows - SS, rows):
        d_copy(b).wait_send()

    def at(dev, e):
        return ys_hbm.at[pl.ds(pl.multiple_of((dev * experts + e) * many, many), many)]

    def at_all(dev):
        return ys_hbm.at[pl.ds(pl.multiple_of(dev * experts * many, many), experts * many)]

    def here(slot, e):
        return xbuf.at[slot, pl.ds(pl.multiple_of(e * many, many), many)]

    def l_copy(e):
        return pltpu.make_async_copy(here(0, e), at(me, e), l_sem)

    def c_copy(e):
        return remote(here(0, e), at(me, e), c_ssem, c_rsem, core_peer)

    def p_copy(e):
        return remote(here(0, e), here(1, e), p_ssem, p_rsem.at[e], x_peer)

    def f_copy(e):
        return remote(here(1, e), at(x_peer, e), f_ssem, f_rsem, core_peer)

    def k_copy(e):
        return pltpu.make_async_copy(here(1, e), at(x_peer, e), k_sem)

    def send(e):
        p_copy(e).start()
        c_copy(e).start()
        l_copy(e).start()

    def forward(e):
        p_copy(e).wait_recv()
        f_copy(e).start()
        k_copy(e).start()

    def expert(e, _):
        @pl.when(e >= 1)
        def _():
            send(e - 1)

        @pl.when(e >= LAG)
        def _():
            forward(e - LAG)

        xs = xst[pl.ds(e * per, per)].reshape(many, width)
        acc = None
        for f in range(units):
            u = e * units + f
            slot = u % WS
            w1_copy(u).wait()
            w2_copy(u).wait()
            for k in range(FC // FS):
                cut = slice(k * FS, (k + 1) * FS)
                hid = jnp.dot(xs, w1[slot, :, cut], preferred_element_type=jnp.float32)
                hid = jax.nn.gelu(hid).astype(jnp.bfloat16)
                part = jnp.dot(hid, w2[slot, cut, :], preferred_element_type=jnp.float32)
                acc = part if acc is None else acc + part

            @pl.when(u + WS < experts * units)
            def _():
                w1_copy(u + WS).start()
                w2_copy(u + WS).start()

        xbuf[0, pl.ds(pl.multiple_of(e * many, many), many)] = acc.astype(jnp.bfloat16)
        return 0

    lax.fori_loop(0, experts, expert, 0)
    send(experts - 1)
    for e in range(experts - LAG, experts):
        forward(e)
    remote(qbuf, qbuf, x_ssem, x_rsem.at[0], x_peer).wait_send()
    for z in zc:
        z.wait_send()
    mine, theirs, whole = at_all(me), at_all(x_peer), xbuf.at[0]
    remote(whole, mine, c_ssem, c_rsem, core_peer).wait()
    remote(whole, mine, p_ssem, p_rsem.at[0], x_peer).wait_send()
    remote(whole, theirs, f_ssem, f_rsem, core_peer).wait()
    pltpu.make_async_copy(whole, mine, l_sem).wait()
    pltpu.make_async_copy(whole, theirs, k_sem).wait()


def _combine_kernel(len_ref, ct_hbm, ys_hbm, y_hbm, ysv, ysb, ctb, yb, ys_sem, ct_sem, y_sem):
    rows, toks, width = y_hbm.shape
    slots = ys_hbm.shape[0]
    start = lax.axis_index("seq") * toks

    def ys_copy(h):
        return pltpu.make_async_copy(ys_hbm.at[:, pl.ds(pl.multiple_of(h * G, G), G)], ysv.at[h], ys_sem.at[h])

    def ct_copy(b):
        return pltpu.make_async_copy(ct_hbm.at[b], ctb.at[b % YS], ct_sem.at[b % YS])

    def y_copy(b):
        return pltpu.make_async_copy(yb.at[b % YS], y_hbm.at[b], y_sem.at[b % YS])

    ys_copy(0).start()
    for k in range(YS - 2):
        ct_copy(k).start()
    for h in range(1, rows // G):
        ys_copy(h).start()
    swap = _swap_matrix()

    def half(h, _):
        ys_copy(h).wait()
        for g in range(slots // G):
            blk = ysv[h, pl.ds(g * G, G)].reshape(G * G, width)
            out = jnp.dot(swap, blk, preferred_element_type=jnp.float32).astype(jnp.bfloat16)
            ysb[:, pl.ds(g * G, G), :] = out.reshape(G, G, width)

        def pair(p, _):
            first = h * G + 2 * p
            limits = []
            for j in range(2):
                b = first + j

                @pl.when(b + YS - 2 < rows)
                def _():
                    ct_copy(b + YS - 2).start()

                ct_copy(b).wait()

                @pl.when(b >= YS)
                def _():
                    y_copy(b - YS).wait()

                limits.append(len_ref[b] - start)

            @pl.when(jnp.maximum(limits[0], limits[1]) > 0)
            def _():
                for j in range(2):
                    slot = (first + j) % YS
                    own = ysb[2 * p + j]
                    for k in range(toks // BLK):
                        c = ctb[slot, :, k * BLK:(k + 1) * BLK]
                        mixed = lax.dot_general(c, own, (((0,), (0,)), ((), ())),
                                                preferred_element_type=jnp.float32)
                        pos = lax.broadcasted_iota(jnp.int32, (BLK, 1), 0) + k * BLK
                        yb[slot, k * BLK:(k + 1) * BLK, :] = jnp.where(
                            pos < limits[j], mixed, 0.0).astype(jnp.bfloat16)

            @pl.when(jnp.maximum(limits[0], limits[1]) <= 0)
            def _():
                for j in range(2):
                    yb[(first + j) % YS] = jnp.zeros((toks, width), jnp.bfloat16)

            for j in range(2):
                y_copy(first + j).start()
            return 0

        lax.fori_loop(0, G // 2, pair, 0)
        return 0

    lax.fori_loop(0, rows // G, half, 0)

    def finish(b, _):
        y_copy(b).wait()
        return 0
    lax.fori_loop(rows - YS, rows, finish, 0)


def solution(mesh):
    def shard_body(tok_blk, len_blk, slot_params, logit_scale, w_in_blk, w_out_blk):
        rows, toks, width = tok_blk.shape
        slots = slot_params.shape[1]
        experts, _, ff = w_in_blk.shape
        own = slots // mesh.shape["seq"]
        per = own // experts
        bf, f32 = jnp.bfloat16, jnp.float32
        any_spec = pl.BlockSpec(memory_space=pl.ANY)
        smem = pl.BlockSpec(memory_space=pltpu.SMEM)
        dma = pltpu.SemaphoreType.DMA
        ys, ct = pl.pallas_call(
            functools.partial(_front_kernel, rows, experts),
            out_shape=(jax.ShapeDtypeStruct((slots * rows, width), bf),
                       jax.ShapeDtypeStruct((rows, slots, toks), bf)),
            in_specs=[smem, smem, any_spec, any_spec, any_spec, any_spec],
            out_specs=(any_spec, any_spec),
            scratch_shapes=[
                pltpu.VMEM((TS, toks, width), bf),
                pltpu.VMEM((width, slots), bf),
                pltpu.VMEM((slots, width), bf),
                pltpu.VMEM((slots, toks), bf),
                pltpu.VMEM((2, slots, toks), bf),
                pltpu.VMEM((SS, 2, 2, own, width), bf),
                pltpu.VMEM((rows, 2, own, width), bf),
                pltpu.VMEM((rows, own, width), bf),
                pltpu.VMEM((own, rows, width), bf),
                pltpu.VMEM((slots, 128), f32),
                pltpu.VMEM((3, own, 128), f32),
                pltpu.VMEM((128, 128), f32),
                pltpu.VMEM((WS, width, FC), bf),
                pltpu.VMEM((WS, FC, width), bf),
                dma, dma((TS,)), dma((2,)), dma((WS, 2)), dma((3,)), dma((3,)),
                dma((SS,)), dma((rows,)), dma, dma((rows // G,)),
                dma, dma, dma, dma, dma, dma((experts,)), dma, dma,
            ],
            compiler_params=pltpu.CompilerParams(
                collective_id=0, has_side_effects=True, vmem_limit_bytes=67_000_000),
            name="front",
        )(len_blk, logit_scale, slot_params, tok_blk, w_in_blk, w_out_blk)
        return pl.pallas_call(
            _combine_kernel,
            in_specs=[smem, any_spec, any_spec],
            out_specs=any_spec,
            out_shape=jax.ShapeDtypeStruct((rows, toks, width), bf),
            scratch_shapes=[
                pltpu.VMEM((rows // G, slots, G, width), bf),
                pltpu.VMEM((G, slots, width), bf),
                pltpu.VMEM((YS, slots, toks), bf),
                pltpu.VMEM((YS, toks, width), bf),
                dma((rows // G,)), dma((YS,)), dma((YS,)),
            ],
            compiler_params=pltpu.CompilerParams(vmem_limit_bytes=60_000_000),
            name="combine",
        )(len_blk, ct, ys.reshape(slots, rows, width))

    return jax.shard_map(
        shard_body,
        mesh=mesh,
        in_specs=(P("data", "seq", None), P("data"), P(None, None), P(None), P("seq", None, None), P("seq", None, None)),
        out_specs=P("data", "seq", None),
        check_vma=False,
    )
```
